32 devices in a mesh: rep: 2 (over y), tp: 4 (over z), ep: 4 (over x, core).
Axes of the slice: x: 2, y: 2, z: 4, core: 2. Of those that a mesh axis runs over, the one named last changes fastest.
Arguments:
- tokens: bfloat16 [768, 3072], P(('rep', 'ep'), 'tp'), parts along dimension 0, may hold values from -6 to 6
- routing: int32 [768, 2], P(('rep', 'ep')), parts along dimension 0, may hold values from 0 to 3, all different within a row; in each aligned block of 96 rows (0 to 95, 96 to 191, ...) at most 54 rows name the same one
- route_gates: float32 [768, 2], P(('rep', 'ep')), parts along dimension 0, may hold values from 0.2 to 1
- expert_gate: bfloat16 [4, 3072, 8192], P('ep', None, 'tp'), may hold values from -0.109375 to 0.109375
- expert_up: bfloat16 [4, 3072, 8192], P('ep', None, 'tp'), may hold values from -0.109375 to 0.109375
- expert_down: bfloat16 [4, 8192, 3072], P('ep', 'tp'), may hold values from -0.0625 to 0.0625
Outputs:
- mixture: bfloat16 [768, 3072], P(('rep', 'ep'), 'tp'), parts along dimension 0
The draws below stay inside these ranges and needn't reach their ends.
There are 2 independent parts, one for each index of `rep`. The reference program is written for one: setup_inputs(seed, part) draws one part's arguments, and reference() takes and returns one part's arrays. A program takes and returns all parts, laid end to end along the dimension named above; an argument that names none is the same for every part. Nothing has to cross between parts.
Inputs may be any that keep to these rules, and one draw needn't show every extreme that they name: `routing`: each token names two different experts. In each aligned block of 96 tokens (the rows of one index of ep) no expert is named by more than 54 tokens, a bound that some block reaches.
All inputs are finite; a program needn't handle non-finite values.
Results may differ from the reference program's by a relative error of at most 0.0085.
Values may be sent and summed in bfloat16 or wider, within the bound.
A program may use at most 128 MiB of HBM per device.

```python
import math
import jax
import jax.numpy as jnp
import numpy as np
from jax import lax

D = 3072
FF = 8192
TOK_DEV = 96
EXPERTS = 4
CAP = 54
TOKENS = 384


def shard_levels(key, extent, split, least, top_value):
    factor_of, own = 1.0, jax.random.fold_in(key, 6)
    for dim, blocks in split:
        draws = jnp.exp(jax.random.uniform(jax.random.fold_in(own, dim), (blocks,), jnp.float32, least / len(split), top_value / len(split)))
        factor_of = factor_of * jnp.repeat(draws, extent[dim] // blocks).reshape([-1 if axis == dim else 1 for axis in range(len(extent))])
    return factor_of


def routed_block(rng, own, number, rows, number_of, top, limit, slope):
    order = jax.random.permutation(rng, number_of)
    heavy_load, ordinary = load_shares(number_of, rows * top, limit, slope, True), load_shares(number_of, rows * top, limit, slope, False)
    places = jnp.arange(number_of)

    def named(sizes, offset_by):
        used = int((sizes > 0).sum())
        fixed = max(1, used // 4)
        moved = fixed + (places - fixed + offset_by * (used - fixed)) % max(1, number_of - fixed)
        return jnp.zeros((number_of,), jnp.int32).at[order[jnp.where(places < fixed, places, moved)]].set(jnp.asarray(sizes, jnp.int32))

    sizes = jnp.where(number % 4 == 0, named(heavy_load, number // 4), named(ordinary, number - number // 4 - 1))
    mixed = jax.random.permutation(jax.random.fold_in(own, 3), number_of)
    giver, sink = mixed[0:number_of // 2 * 2:2], mixed[1:number_of // 2 * 2:2]
    room = jnp.minimum(sizes[giver] - 1, limit - sizes[sink]) // 2
    room = jnp.where((giver == order[0]) | (sink == order[0]) | (sizes[sink] == 0), 0, jnp.maximum(room, 0))
    moved = jax.random.randint(jax.random.fold_in(own, 4), (number_of // 2,), 0, 1 << 20) % (room + 1)
    sizes = sizes.at[giver].add(-moved).at[sink].add(moved)
    members = jnp.searchsorted(jnp.cumsum(sizes), jnp.arange(rows * top), side="right").astype(jnp.int32)
    grid = members.reshape(top, rows).T
    grid = grid[jax.random.permutation(jax.random.fold_in(own, 1), rows)]
    offset_by = jax.random.randint(jax.random.fold_in(own, 2), (rows, 1), 0, top)
    return jnp.take_along_axis(grid, (jnp.arange(top)[None, :] + offset_by) % top, axis=1)


def load_shares(number_of, total, most, slope, full):
    portions = [(1 << 20) // math.isqrt(rank ** slope) + 1 for rank in range(1, number_of + 1)]
    largest = most if full else min(most, max(-(-total // number_of), total * portions[0] // sum(portions)))
    least = 1 if total - largest >= number_of - 1 else 0
    holding, spare = [largest] + [least] * (number_of - 1), total - largest - least * (number_of - 1)
    while spare > 0:
        movable = [i for i in range(1, number_of) if holding[i] < largest] or [i for i in range(1, number_of) if holding[i] < most]
        mass, remaining = sum([portions[i] for i in movable]), spare
        for i in movable:
            addition = min(most - holding[i], max(1, remaining * portions[i] // mass), spare)
            holding[i] = holding[i] + addition
            spare = spare - addition
    return np.array(holding)


def gaussian(stream_key, extent, scale, most, cuts=(), held_as=jnp.bfloat16):
    result = jax.random.normal(stream_key, extent, jnp.float32) * scale
    if len(cuts) > 0:
        result = shard_levels(stream_key, extent, cuts, -0.22, 0.18) * result
    return jnp.clip(result, min=-most, max=most).astype(held_as)


def setup_inputs(seed: int = 0, part: int = 0) -> dict:
    seeds = jax.random.split(jax.random.key(seed), 7)
    part_splits = jax.random.split(jax.random.fold_in(seeds[6], part), 7)
    tokens = gaussian(part_splits[0], (TOKENS, D), 1.0, 6.0, ((0, 4), (1, 4)))
    routing_keys = jax.random.split(jax.random.fold_in(part_splits[1], 1), TOKENS // TOK_DEV)
    routing_turns = jax.random.permutation(jax.random.fold_in(part_splits[1], 3), TOKENS // TOK_DEV)
    routing = jax.vmap(lambda own, number: routed_block(jax.random.fold_in(part_splits[1], 2), own, number, TOK_DEV, EXPERTS, 2, CAP, 2))(routing_keys, routing_turns).reshape((TOKENS, 2))
    route_gates = jnp.clip(0.2 + 0.8 * jax.random.uniform(part_splits[2], (TOKENS, 2), jnp.float32) ** shard_levels(part_splits[2], (TOKENS, 2), ((0, 4),), -0.2, 0.2), 0.2, 1.0)
    expert_gate = gaussian(seeds[3], (EXPERTS, D, FF), D ** -0.5, 0.109375, ((0, 4), (2, 4)))
    expert_up = gaussian(seeds[4], (EXPERTS, D, FF), D ** -0.5, 0.109375, ((0, 4), (2, 4)))
    expert_down = gaussian(seeds[5], (EXPERTS, FF, D), FF ** -0.5, 0.0625, ((0, 4), (1, 4)))
    return {"tokens": tokens, "routing": routing, "route_gates": route_gates, "expert_gate": expert_gate, "expert_up": expert_up, "expert_down": expert_down}


def slot_tables(routing, route_gates):
    count_rows = routing.shape[0]
    choices_n = routing.shape[1]
    flat_ids = routing.reshape(-1).astype(jnp.int32)
    onehot = (flat_ids[:, None] == jnp.arange(EXPERTS, dtype=jnp.int32)[None, :]).astype(jnp.int32)
    before = jnp.cumsum(onehot, axis=0) - onehot
    position = jnp.sum(before * onehot, axis=1)
    slot_index = flat_ids * CAP + position
    picked = (slot_index[:, None] == jnp.arange(EXPERTS * CAP, dtype=jnp.int32)[None, :]).astype(jnp.float32)
    dispatch = picked.reshape(count_rows, choices_n, EXPERTS * CAP).sum(axis=1)
    combine = (picked * route_gates.reshape(-1)[:, None]).reshape(count_rows, choices_n, EXPERTS * CAP).sum(axis=1)
    return dispatch, combine


def one_expert(operands):
    row_block, w_gate, w_upward, w_down = operands
    gate_part = jnp.dot(row_block, w_gate, preferred_element_type=jnp.float32)
    upward = jnp.dot(row_block, w_upward, preferred_element_type=jnp.float32)
    hidden = (jax.nn.silu(gate_part) * upward).astype(jnp.bfloat16)
    return jnp.dot(hidden, w_down, preferred_element_type=jnp.float32).astype(jnp.bfloat16)


def reference(tokens, routing, route_gates, expert_gate, expert_up, expert_down):
    blocks = TOKENS // TOK_DEV
    dispatch, combine = jax.vmap(slot_tables)(routing.reshape(blocks, TOK_DEV, 2), route_gates.reshape(blocks, TOK_DEV, 2))
    block_tokens = tokens.reshape(blocks, TOK_DEV, D).astype(jnp.float32)
    packed = jnp.einsum('btc,btd->bcd', dispatch, block_tokens, precision=lax.Precision.HIGHEST).astype(jnp.bfloat16)
    expert_rows = packed.reshape(blocks, EXPERTS, CAP, D).transpose(1, 0, 2, 3).reshape(EXPERTS, blocks * CAP, D)
    expert_out = lax.map(one_expert, (expert_rows, expert_gate, expert_up, expert_down))
    back = expert_out.reshape(EXPERTS, blocks, CAP, D).transpose(1, 0, 2, 3).reshape(blocks, EXPERTS * CAP, D)
    mixed = jnp.einsum('btc,bcd->btd', combine, back.astype(jnp.float32), precision=lax.Precision.HIGHEST)
    return mixed.reshape(TOKENS, D).astype(jnp.bfloat16)
```

```python
import functools

import jax
import jax.numpy as jnp
from jax import lax
from jax.experimental import pallas as pl
from jax.experimental.pallas import tpu as pltpu
from jax.sharding import PartitionSpec as P


def slot_tables(routing, route_gates, experts, capacity):
    count_rows = routing.shape[0]
    choices_n = routing.shape[1]
    flat_ids = routing.reshape(-1)
    onehot = (flat_ids[:, None] == jnp.arange(experts, dtype=jnp.int32)[None, :]).astype(jnp.int32)
    before = jnp.cumsum(onehot, axis=0) - onehot
    position = jnp.sum(before * onehot, axis=1)
    slot_index = flat_ids * capacity + position
    picked = (
        slot_index[:, None] == jnp.arange(experts * capacity, dtype=jnp.int32)[None, :]
    ).astype(jnp.float32)
    dispatch = picked.reshape(count_rows, choices_n, experts * capacity).sum(axis=1)
    combine = (
        (picked * route_gates.reshape(-1)[:, None])
        .reshape(count_rows, choices_n, experts * capacity)
        .sum(axis=1)
    )
    return (dispatch, combine)


def hidden_rows(everyone, expert_gate, expert_up, capacity):
    local_count = expert_gate.shape[0]
    total = everyone.shape[0]
    row_block = everyone.reshape(
        total // (local_count * capacity), local_count, capacity, everyone.shape[1]
    )
    gate_part = jnp.einsum(
        "tlcd,ldf->tlcf", row_block, expert_gate, preferred_element_type=jnp.float32
    )
    upward = jnp.einsum("tlcd,ldf->tlcf", row_block, expert_up, preferred_element_type=jnp.float32)
    return (jax.nn.silu(gate_part) * upward).astype(jnp.bfloat16)


def plain_body(tokens, routing, route_gates, expert_gate, expert_up, expert_down):
    local_count = expert_gate.shape[0]
    ep_count = lax.axis_size("ep")
    tp_count = lax.axis_size("tp")
    tok_count = tokens.shape[0]
    capacity = 2 * tok_count // ep_count + tok_count // 16
    experts = local_count * ep_count
    dispatch, combine = slot_tables(routing, route_gates, experts, capacity)
    dispatch_low = dispatch.astype(jnp.bfloat16)
    whole = lax.all_gather(tokens, "tp", axis=1, tiled=True)
    packed = jnp.einsum(
        "tc,td->cd", dispatch_low, whole, preferred_element_type=jnp.float32
    ).astype(jnp.bfloat16)
    everyone = lax.all_to_all(packed, "ep", split_axis=0, concat_axis=0, tiled=True)
    total_rows = everyone.shape[0]
    columns = everyone.shape[1]
    hidden = hidden_rows(everyone, expert_gate, expert_up, capacity)
    part = jnp.einsum("tlcf,lfd->dtlc", hidden, expert_down, preferred_element_type=jnp.float32)
    summed_t = lax.psum_scatter(
        part.reshape(columns // tp_count * lax.axis_size("tp"), total_rows),
        "tp",
        scatter_dimension=0,
        tiled=True,
    )
    summed = summed_t.T
    expert_out = summed.astype(jnp.bfloat16)
    returned = lax.all_to_all(expert_out, "ep", split_axis=0, concat_axis=0, tiled=True)
    mixed = jnp.dot(combine, returned.astype(jnp.float32), precision=lax.Precision.HIGHEST)
    return mixed.astype(jnp.bfloat16)


MESH = pl.DeviceIdType.MESH
LANES = 128


def up_to(value, step):
    return -(-value // step) * step


def rcopy(src, dst, send, recv, device):
    return pltpu.make_async_remote_copy(
        src_ref=src, dst_ref=dst, send_sem=send, recv_sem=recv, device_id=device, device_id_type=MESH
    )


def layer_kernel(
    tp, ep, cap, rows, tokens, routing, gates, gate_hbm, up_hbm, down_hbm, out,
    x, m, m_own, pick, place, scale, wg, wu, wd, acc_g, acc_u, packed, hidden,
    c, c_in, x_out, x_in, z_out, z_in,
    t_sem, w_sem, zs, zr, xs, xr, cs, cr, ms, mr, rcs, rcr, rxs, rxr, rzs, rzr,
):
    t = lax.axis_index("tp")
    e = lax.axis_index("ep")
    half = ep // 2
    core = lax.rem(e, 2)
    column = e // 2
    e_core = e + 1 - 2 * core
    e_x = lax.rem(e + half, ep)
    e_xc = lax.rem(e_core + half, ep)
    tok, feat = tokens.shape
    ff = wg.shape[2]
    f32, b16 = jnp.float32, jnp.bfloat16
    to_x, to_core = {"ep": e_x}, {"ep": e_core}
    above, below = {"tp": lax.rem(t + 1, tp)}, {"tp": lax.rem(t + tp - 1, tp)}

    barrier = pltpu.get_barrier_semaphore()

    @pl.when(t < tp - 1)
    def _():
        pl.semaphore_signal(barrier, inc=1, device_id=above, device_id_type=MESH)

    @pl.when(t > 0)
    def _():
        pl.semaphore_signal(barrier, inc=1, device_id=below, device_id_type=MESH)

    pl.semaphore_signal(barrier, inc=1, device_id=to_x, device_id_type=MESH)
    pl.semaphore_signal(barrier, inc=1, device_id=to_core, device_id_type=MESH)

    own_load = pltpu.make_async_copy(tokens, x.at[t, e, pl.ds(0, tok), :], t_sem.at[0])
    own_load.start()

    def select(values):
        found = jnp.int32(values[0])
        for k in range(1, tp):
            found = jnp.where(t == k, jnp.int32(values[k]), found)
        return found

    def near(k):
        return sorted(range(tp), key=lambda q: (abs(q - k), q))

    def far(k):
        return sorted(range(tp), key=lambda q: (-abs(q - k), abs(2 * q - tp + 1), q))

    arrivals = [select([near(k)[i] for k in range(tp)]) for i in range(tp)]
    leaving = [select([far(k)[i] for k in range(tp)]) for i in range(tp)]
    pieces = 2 if tok % 32 == 0 else 1
    piece = tok // pieces

    loads = []
    for d in range(tp):
        q = arrivals[d]
        for k, (src, dst) in enumerate(((gate_hbm, wg), (up_hbm, wu))):
            r = pl.ds(pl.multiple_of(q * feat, feat), feat)
            loads.append(pltpu.make_async_copy(src.at[0, r, :], dst.at[q], w_sem.at[k * tp + d]))
    down_loads = []
    for i in range(tp):
        q = leaving[i]
        r = pl.ds(pl.multiple_of(q * feat, feat), feat)
        down_loads.append(pltpu.make_async_copy(down_hbm.at[0, :, r], wd.at[q], w_sem.at[2 * tp + i]))
    pad = x.shape[2] - tok
    for q in range(tp):
        for b in range(ep):
            x[q, b, tok:, :] = jnp.zeros((pad, feat), b16)
    m_own[...] = jnp.full(m_own.shape, -1.0, f32)
    m_own[0:2, 0:tok] = routing[...].astype(f32)
    m_own[2:4, 0:tok] = gates[...]
    m[e] = m_own[...]

    own_load.wait()
    for load in loads + down_loads:
        load.start()
    pl.semaphore_wait(barrier, 2 + jnp.where(t > 0, 1, 0) + jnp.where(t < tp - 1, 1, 0))

    sent = []

    def send(src, dst, s, r, device):
        copy = rcopy(src, dst, s, r, device)
        copy.start()
        sent.append((None, copy))

    def block(q, b, p):
        return x.at[q, b, pl.ds(p * piece, piece), :]

    def send_if(cond, src, dst, s, r, device):
        copy = rcopy(src, dst, s, r, device)
        sent.append((cond, copy))

        @pl.when(cond)
        def _():
            copy.start()

    for p in range(pieces):
        n = pieces * t + p
        own = block(t, e, p)
        send_if(t < tp - 1, own, own, zs.at[n], zr.at[n], above)
        send_if(t > 0, own, own, zs.at[pieces * tp + n], zr.at[n], below)
        send(own, own, xs.at[n], xr.at[n], to_x)
        if p == 0:
            send(m_own, m.at[e], ms.at[0], mr.at[0], to_x)
            send(m_own, m.at[e], ms.at[1], mr.at[1], to_core)
        send(own, own, cs.at[n], cr.at[n], to_core)

    def got(dst, s, r, device):
        rcopy(dst, dst, s, r, device).wait_recv()

    def take_z(d, ps):
        for up in (True, False):
            q = t - d if up else t + d
            here = q >= 0 if up else q < tp
            onward = here & (t < tp - 1) if up else here & (t > 0)
            away = above if up else below
            q = jnp.clip(q, 0, tp - 1)
            for p in ps:
                n = pieces * q + p
                one = block(q, e, p)
                k = n if up else pieces * tp + n

                @pl.when(here)
                def _(one=one, n=n):
                    got(one, zs.at[n], zr.at[n], away)

                send_if(onward, one, one, zs.at[k], zr.at[n], away)
                send_if(here, one, one, xs.at[n], xr.at[n], to_x)
                send_if(here, one, one, cs.at[n], cr.at[n], to_core)

    def take_x(i):
        for p in range(pieces):
            n = pieces * arrivals[i] + p
            far_n = pieces * tp + n
            one = block(arrivals[i], e_x, p)
            got(one, xs.at[n], xr.at[n], to_x)
            send(one, one, cs.at[far_n], cr.at[far_n], to_core)

    def take_core(i):
        for p in range(pieces):
            n = pieces * arrivals[i] + p
            far_n = pieces * tp + n
            got(block(arrivals[i], e_core, p), cs.at[n], cr.at[n], to_core)
            got(block(arrivals[i], e_xc, p), cs.at[far_n], cr.at[far_n], to_core)

    got(m.at[e_x], ms.at[0], mr.at[0], to_x)
    send(m.at[e_x], m.at[e_x], ms.at[2], mr.at[2], to_core)
    got(m.at[e_core], ms.at[1], mr.at[1], to_core)
    got(m.at[e_xc], ms.at[2], mr.at[2], to_core)

    slots = pick.shape[0]
    mine = e.astype(f32)
    earlier = (
        lax.broadcasted_iota(jnp.int32, (LANES, LANES), 0)
        < lax.broadcasted_iota(jnp.int32, (LANES, LANES), 1)
    ).astype(b16)
    slot = lax.broadcasted_iota(jnp.int32, (slots, LANES), 0).astype(f32)
    total = jnp.zeros((slots, 1), f32)
    for b in range(ep):
        first, second = m[b, 0:1, :] == mine, m[b, 1:2, :] == mine
        named = jnp.where(first, 1.0, 0.0) + jnp.where(second, 1.0, 0.0)
        weight = jnp.where(first, m[b, 2:3, :], 0.0) + jnp.where(second, m[b, 3:4, :], 0.0)
        spread = jnp.broadcast_to(named, (16, LANES)).astype(b16)
        position = jnp.dot(spread, earlier, preferred_element_type=f32)[0:1, :]
        where_to = jnp.where(named > 0.5, position + float(b * cap), -1.0)
        chosen = jnp.where(slot == where_to, 1.0, 0.0)
        total = total + jnp.sum(chosen * weight, axis=1, keepdims=True)
        pick[:, b * LANES:(b + 1) * LANES] = chosen.astype(b16)
        at = ((b % 2) * half + b // 2) * tok
        place[at:at + tok, :] = chosen.T[0:tok, :].astype(b16)
    scale[...] = jnp.broadcast_to(total, scale.shape)

    step = 1024 if ff % 1024 == 0 else 512
    tiles = ff // step

    def project(d, last):
        q = arrivals[d]
        loads[2 * d].wait()
        loads[2 * d + 1].wait()
        everyone = x[q].reshape(ep * x.shape[2], feat)
        packed[...] = jnp.dot(pick[0:rows, :], everyone, preferred_element_type=f32).astype(b16)

        def tile(j, carry):
            cols = pl.ds(pl.multiple_of(j * step, step), step)
            g = jnp.dot(packed[...], wg[q, :, cols], preferred_element_type=f32)
            u = jnp.dot(packed[...], wu[q, :, cols], preferred_element_type=f32)
            if d > 0:
                g = g + acc_g[:, cols]
                u = u + acc_u[:, cols]
            if last:
                h = g / (1.0 + jnp.exp(-g)) * u * scale[0:rows, 0:1]
                hidden[:, cols] = h.astype(b16)
            else:
                acc_g[:, cols] = g
                acc_u[:, cols] = u
            return carry

        lax.fori_loop(0, tiles, tile, 0)

    take_z(1, range(pieces))
    take_x(0)
    take_core(0)
    take_z(2, range(pieces))
    take_x(1)
    project(0, False)
    take_core(1)
    for d in range(3, tp):
        take_z(d, range(pieces - 1))
    project(1, False)
    for d in range(3, tp):
        take_z(d, range(pieces - 1, pieces))
    for i in range(2, tp):
        take_x(i)
        take_core(i)
        project(i, i == tp - 1)

    width = 256 if feat % 256 == 0 else LANES
    tail = jnp.zeros((slots - rows, width), b16)

    def leaves(i):
        q = leaving[0]
        for k in range(1, tp):
            q = jnp.where(i == k, leaving[k], q)
        return q

    def down_load(i):
        r = pl.ds(pl.multiple_of(leaves(i) * feat, feat), feat)
        return pltpu.make_async_copy(down_hbm.at[0, :, r], wd.at[leaves(i)], w_sem.at[2 * tp + i])

    def to_partner(i):
        away = pl.ds((1 - core) * half, half)
        return rcopy(c.at[i, away], c_in.at[i], rcs.at[i], rcr.at[i], to_core)

    def to_tokens(i):
        q = leaves(i)
        down_load(i).wait()
        for j in range(feat // width):
            cols = slice(j * width, (j + 1) * width)
            part = jnp.dot(hidden[...], wd[q, :, cols], preferred_element_type=f32).astype(b16)
            part = jnp.concatenate([part, tail], axis=0) if slots > rows else part
            back = jnp.dot(place[...], part, preferred_element_type=f32).astype(b16)
            c[i, :, :, cols] = back.reshape(ep, tok, width)
        to_partner(i).start()

    def part_of(p):
        return slice(p * piece, (p + 1) * piece)

    def to_other_x(i, p):
        n, view = pieces * i + p, pl.ds(p * piece, piece)
        return rcopy(x_out.at[i, view], x_in.at[i, view], rxs.at[n], rxr.at[n], to_x)

    def sum_core(i):
        got(c_in.at[i], rcs.at[i], rcr.at[i], to_core)
        other = 1 - column
        for p in range(pieces):
            r = part_of(p)
            value = c[i, core * half + other, r].astype(f32) + c_in[i, other, r].astype(f32)
            x_out[i, r] = value.astype(b16)
            to_other_x(i, p).start()

    def sum_x(i, p):
        r, n = part_of(p), pieces * i + p
        got(x_in.at[i, pl.ds(p * piece, piece)], rxs.at[n], rxr.at[n], to_x)
        value = c[i, core * half + column, r].astype(f32) + c_in[i, column, r].astype(f32)
        return value + x_in[i, r].astype(f32)

    def pass_on(i, p):
        q = leaving[i]
        right = q > t
        view = pl.ds(p * piece, piece)
        value = sum_x(i, p)
        behind = (right & (t > 0)) | (~right & (t < tp - 1))
        n_in = pieces * q + p

        @pl.when(behind)
        def _():
            got(z_in.at[q, view], rzs.at[0], rzr.at[n_in], above)
            z_out[i, part_of(p)] = (value + z_in[q, part_of(p)].astype(f32)).astype(b16)

        @pl.when(~behind)
        def _():
            z_out[i, part_of(p)] = value.astype(b16)

        slot_to = jnp.where(~right & (q == t - 1), tp, q)
        peer = {"tp": jnp.where(right, lax.rem(t + 1, tp), lax.rem(t + tp - 1, tp))}
        send(
            z_out.at[i, view], z_in.at[slot_to, view],
            rzs.at[pieces * i + p], rzr.at[pieces * slot_to + p], peer,
        )

    to_tokens(0)

    def following(i, carry):
        to_tokens(i)
        sum_core(i - 1)
        return carry

    lax.fori_loop(1, tp, following, 0)
    sum_core(tp - 1)
    for i in range(tp):
        sent.append((None, to_partner(i)))
        for p in range(pieces):
            sent.append((None, to_other_x(i, p)))
    for p in range(pieces):
        pass_on(0, p)
    for p in range(pieces):
        for i in range(1, tp - 1):
            pass_on(i, p)
    for p in range(pieces):
        view = pl.ds(p * piece, piece)
        result = sum_x(tp - 1, p)
        acc_g[part_of(p), 0:feat] = result
        for cond, at in ((t > 0, t), (t < tp - 1, tp)):

            @pl.when(cond)
            def _(at=at):
                got(z_in.at[at, view], rzs.at[0], rzr.at[pieces * at + p], above)
                acc_g[part_of(p), 0:feat] += z_in[at, part_of(p)].astype(f32)

        out[part_of(p), :] = acc_g[part_of(p), 0:feat].astype(b16)
    for cond, copy in sent:
        if cond is None:
            copy.wait_send()
        else:

            @pl.when(cond)
            def _(copy=copy):
                copy.wait_send()


def kernel_body(tokens, routing, route_gates, expert_gate, expert_up, expert_down):
    ep, tp = lax.axis_size("ep"), lax.axis_size("tp")
    tok, feat = tokens.shape
    ff = expert_gate.shape[2]
    cap = 2 * tok // ep + tok // 16
    rows = up_to(ep * cap, 16)
    slots = up_to(rows, LANES)
    f32, b16 = jnp.float32, jnp.bfloat16
    dma = pltpu.SemaphoreType.DMA
    vmem = pl.BlockSpec(memory_space=pltpu.VMEM)
    hbm = pl.BlockSpec(memory_space=pl.ANY)
    return pl.pallas_call(
        functools.partial(layer_kernel, tp, ep, cap, rows),
        out_shape=pltpu.VMEM((tok, feat), b16),
        in_specs=[hbm, vmem, vmem, hbm, hbm, hbm],
        out_specs=vmem,
        scratch_shapes=[
            pltpu.VMEM((tp, ep, LANES, feat), b16),
            pltpu.VMEM((ep, 8, LANES), f32),
            pltpu.VMEM((8, LANES), f32),
            pltpu.VMEM((slots, ep * LANES), b16),
            pltpu.VMEM((ep * tok, slots), b16),
            pltpu.VMEM((slots, LANES), f32),
            pltpu.VMEM((tp, feat, ff), b16),
            pltpu.VMEM((tp, feat, ff), b16),
            pltpu.VMEM((tp, ff, feat), b16),
            pltpu.VMEM((rows, ff), f32),
            pltpu.VMEM((rows, ff), f32),
            pltpu.VMEM((rows, feat), b16),
            pltpu.VMEM((rows, ff), b16),
            pltpu.VMEM((tp, ep, tok, feat), b16),
            pltpu.VMEM((tp, ep // 2, tok, feat), b16),
            pltpu.VMEM((tp, tok, feat), b16),
            pltpu.VMEM((tp, tok, feat), b16),
            pltpu.VMEM((tp, tok, feat), b16),
            pltpu.VMEM((tp + 1, tok, feat), b16),
            dma((1,)),
            dma((3 * tp,)),
            dma((4 * tp,)), dma((2 * tp,)),
            dma((2 * tp,)), dma((2 * tp,)),
            dma((4 * tp,)), dma((4 * tp,)),
            dma((3,)), dma((3,)),
            dma((tp,)), dma((tp,)),
            dma((2 * tp,)), dma((2 * tp,)),
            dma((2 * tp,)), dma((2 * tp + 2,)),
        ],
        compiler_params=pltpu.CompilerParams(
            collective_id=0, has_side_effects=True, vmem_limit_bytes=60 * 1024 * 1024
        ),
    )(tokens, routing.T, route_gates.T, expert_gate, expert_up, expert_down)


def body(tokens, routing, route_gates, expert_gate, expert_up, expert_down):
    ep, tp = lax.axis_size("ep"), lax.axis_size("tp")
    tok, feat = tokens.shape
    ff = expert_gate.shape[2]
    fits = ep == 4 and tp > 2 and expert_gate.shape[0] == 1 and tok <= LANES and tok % 16 == 0
    fits = fits and feat % LANES == 0 and ff % 512 == 0 and 3 * tp * feat * ff * 2 <= 40 << 20
    run = kernel_body if fits else plain_body
    return run(tokens, routing, route_gates, expert_gate, expert_up, expert_down)


def solution(mesh):
    return jax.shard_map(
        body,
        mesh=mesh,
        in_specs=(
            P(("rep", "ep"), "tp"),
            P(("rep", "ep"), None),
            P(("rep", "ep"), None),
            P("ep", None, "tp"),
            P("ep", None, "tp"),
            P("ep", "tp", None),
        ),
        out_specs=P(("rep", "ep"), "tp"),
        check_vma=False,
    )
```

```python
import functools

import jax
import jax.numpy as jnp
from jax import lax
from jax.experimental import pallas as pl
from jax.experimental.pallas import tpu as pltpu
from jax.sharding import PartitionSpec as P


def slot_tables(routing, route_gates, experts, capacity):
    count_rows = routing.shape[0]
    choices_n = routing.shape[1]
    flat_ids = routing.reshape(-1)
    onehot = (flat_ids[:, None] == jnp.arange(experts, dtype=jnp.int32)[None, :]).astype(jnp.int32)
    before = jnp.cumsum(onehot, axis=0) - onehot
    position = jnp.sum(before * onehot, axis=1)
    slot_index = flat_ids * capacity + position
    picked = (
        slot_index[:, None] == jnp.arange(experts * capacity, dtype=jnp.int32)[None, :]
    ).astype(jnp.float32)
    dispatch = picked.reshape(count_rows, choices_n, experts * capacity).sum(axis=1)
    combine = (
        (picked * route_gates.reshape(-1)[:, None])
        .reshape(count_rows, choices_n, experts * capacity)
        .sum(axis=1)
    )
    return (dispatch, combine)


def hidden_rows(everyone, expert_gate, expert_up, capacity):
    local_count = expert_gate.shape[0]
    total = everyone.shape[0]
    row_block = everyone.reshape(
        total // (local_count * capacity), local_count, capacity, everyone.shape[1]
    )
    gate_part = jnp.einsum(
        "tlcd,ldf->tlcf", row_block, expert_gate, preferred_element_type=jnp.float32
    )
    upward = jnp.einsum("tlcd,ldf->tlcf", row_block, expert_up, preferred_element_type=jnp.float32)
    return (jax.nn.silu(gate_part) * upward).astype(jnp.bfloat16)


def plain_body(tokens, routing, route_gates, expert_gate, expert_up, expert_down):
    local_count = expert_gate.shape[0]
    ep_count = lax.axis_size("ep")
    tp_count = lax.axis_size("tp")
    tok_count = tokens.shape[0]
    capacity = 2 * tok_count // ep_count + tok_count // 16
    experts = local_count * ep_count
    dispatch, combine = slot_tables(routing, route_gates, experts, capacity)
    dispatch_low = dispatch.astype(jnp.bfloat16)
    whole = lax.all_gather(tokens, "tp", axis=1, tiled=True)
    packed = jnp.einsum(
        "tc,td->cd", dispatch_low, whole, preferred_element_type=jnp.float32
    ).astype(jnp.bfloat16)
    everyone = lax.all_to_all(packed, "ep", split_axis=0, concat_axis=0, tiled=True)
    total_rows = everyone.shape[0]
    columns = everyone.shape[1]
    hidden = hidden_rows(everyone, expert_gate, expert_up, capacity)
    part = jnp.einsum("tlcf,lfd->dtlc", hidden, expert_down, preferred_element_type=jnp.float32)
    summed_t = lax.psum_scatter(
        part.reshape(columns // tp_count * lax.axis_size("tp"), total_rows),
        "tp",
        scatter_dimension=0,
        tiled=True,
    )
    summed = summed_t.T
    expert_out = summed.astype(jnp.bfloat16)
    returned = lax.all_to_all(expert_out, "ep", split_axis=0, concat_axis=0, tiled=True)
    mixed = jnp.dot(combine, returned.astype(jnp.float32), precision=lax.Precision.HIGHEST)
    return mixed.astype(jnp.bfloat16)


MESH = pl.DeviceIdType.MESH
LANES = 128
WIDE = 256


def up_to(value, step):
    return -(-value // step) * step


def row_spans(tok):
    units = tok // 16
    first = max(1, units // 6)
    second = (units - first + 1) // 2
    sizes = [16 * first, 16 * second, tok - 16 * (first + second)]
    return [(sum(sizes[:k]), sizes[k]) for k in range(3)]


def rcopy(src, dst, send, recv, device):
    return pltpu.make_async_remote_copy(
        src_ref=src, dst_ref=dst, send_sem=send, recv_sem=recv, device_id=device, device_id_type=MESH
    )


def layer_kernel(
    tp, ep, cap, rows, tokens, routing, gates, gate_hbm, up_hbm, down_hbm, out,
    x, m, m_own, pick, place, scale, wg, wu, wd, acc_g, acc_u, packed, hidden,
    c, c_in, x_out, x_in, y_out, y_in, f_out, f_in, z_out, z_in,
    t_sem, w_sem, zs, zr, xs, xr, cs, cr, ms, mr,
    rcs, rcr, rxs, rxr, rys, ryr, rfs, rfr, rzs, rzr,
):
    t = lax.axis_index("tp")
    e = lax.axis_index("ep")
    half = ep // 2
    core = lax.rem(e, 2)
    column = e // 2
    e_core = e + 1 - 2 * core
    e_x = lax.rem(e + half, ep)
    e_xc = lax.rem(e_core + half, ep)
    tok, feat = tokens.shape
    ff = wg.shape[2]
    nt = feat // WIDE
    f32, b16 = jnp.float32, jnp.bfloat16
    to_x, to_core = {"ep": e_x}, {"ep": e_core}
    above, below = {"tp": lax.rem(t + 1, tp)}, {"tp": lax.rem(t + tp - 1, tp)}

    barrier = pltpu.get_barrier_semaphore()

    @pl.when(t < tp - 1)
    def _():
        pl.semaphore_signal(barrier, inc=1, device_id=above, device_id_type=MESH)

    @pl.when(t > 0)
    def _():
        pl.semaphore_signal(barrier, inc=1, device_id=below, device_id_type=MESH)

    pl.semaphore_signal(barrier, inc=1, device_id=to_x, device_id_type=MESH)
    pl.semaphore_signal(barrier, inc=1, device_id=to_core, device_id_type=MESH)

    own_load = pltpu.make_async_copy(tokens, x.at[t, e, pl.ds(0, tok), :], t_sem.at[0])
    own_load.start()

    def select(values):
        found = jnp.int32(values[0])
        for k in range(1, tp):
            found = jnp.where(t == k, jnp.int32(values[k]), found)
        return found

    def near(k):
        return sorted(range(tp), key=lambda q: (abs(q - k), q))

    def far(k):
        return sorted(range(tp), key=lambda q: (-abs(q - k), abs(2 * q - tp + 1), q))

    arrivals = [select([near(k)[i] for k in range(tp)]) for i in range(tp)]
    leaving = [select([far(k)[i] for k in range(tp)]) for i in range(tp)]
    spans = row_spans(tok)
    pieces = len(spans)
    bulk = range(1, pieces)

    loads = []
    for d in range(tp):
        q = arrivals[d]
        for k, (src, dst) in enumerate(((gate_hbm, wg), (up_hbm, wu))):
            r = pl.ds(pl.multiple_of(q * feat, feat), feat)
            loads.append(pltpu.make_async_copy(src.at[0, r, :], dst.at[q], w_sem.at[k * tp + d]))
    down_loads = []
    for i in range(tp):
        q = leaving[i]
        r = pl.ds(pl.multiple_of(q * feat, feat), feat)
        down_loads.append(pltpu.make_async_copy(down_hbm.at[0, :, r], wd.at[q], w_sem.at[2 * tp + i]))
    pad = x.shape[2] - tok
    for q in range(tp):
        for b in range(ep):
            x[q, b, tok:, :] = jnp.zeros((pad, feat), b16)
    m_own[...] = jnp.full(m_own.shape, -1.0, f32)
    m_own[0:2, 0:tok] = routing[...].astype(f32)
    m_own[2:4, 0:tok] = gates[...]
    m[e] = m_own[...]

    edge = (t == 0) | (t == tp - 1)

    @pl.when(t == 0)
    def _():
        y_in[0:tp] = jnp.zeros((tp, *y_in.shape[1:]), b16)
        z_in[0:tp * nt] = jnp.zeros((tp * nt, *z_in.shape[1:]), b16)

    @pl.when(t == tp - 1)
    def _():
        y_in[0:tp - 1] = jnp.zeros((tp - 1, *y_in.shape[1:]), b16)
        y_in[tp] = jnp.zeros(y_in.shape[1:], b16)
        z_in[0:(tp - 1) * nt] = jnp.zeros(((tp - 1) * nt, *z_in.shape[1:]), b16)
        z_in[tp * nt:] = jnp.zeros((nt, *z_in.shape[1:]), b16)

    own_load.wait()
    for load in loads + down_loads:
        load.start()
    pl.semaphore_wait(barrier, 2 + jnp.where(t > 0, 1, 0) + jnp.where(t < tp - 1, 1, 0))

    def send(src, dst, s, r, device):
        rcopy(src, dst, s, r, device).start()

    def block(q, b, p):
        return x.at[q, b, pl.ds(*spans[p]), :]

    def send_if(cond, src, dst, s, r, device):
        @pl.when(cond)
        def _():
            send(src, dst, s, r, device)

    def at(side, q, p):
        return (side * tp + q) * pieces + p

    def up_down(side, q, p, up, cond):
        one = block(q, (e, e_x)[side], p)
        n = at(side, q, p)
        send_if(cond, one, one, zs.at[at(2 * up + side, q, p)], zr.at[n], above if up else below)

    send(m_own, m.at[e], ms.at[0], mr.at[0], to_x)
    send(m_own, m.at[e], ms.at[1], mr.at[1], to_core)
    for p in (*bulk, 0):
        own = block(t, e, p)
        n = at(0, t, p)
        send(own, own, xs.at[n], xr.at[n], to_x)
        up_down(0, t, p, 1, t < tp - 1)
        up_down(0, t, p, 0, t > 0)
        send(own, own, cs.at[n], cr.at[n], to_core)

    def got(dst, s, r, device):
        rcopy(dst, dst, s, r, device).wait_recv()

    def take_z(d, ps, side=0):
        for p in ps:
            for up in (1, 0):
                q = t - d if up else t + d
                here = q >= 0 if up else q < tp
                onward = here & (t < tp - 1 if up else t > 0)
                q = jnp.clip(q, 0, tp - 1)
                one = block(q, (e, e_x)[side], p)
                n = at(side, q, p)

                @pl.when(here)
                def _(one=one, n=n, p=p):
                    got(one, zs.at[0], zr.at[n], above)
                    if p > 0:
                        send(one, one, xs.at[n], xr.at[n], to_x)
                    send(one, one, cs.at[n], cr.at[n], to_core)

                up_down(side, q, p, up, onward)

    def take_x(i, ps):
        q = arrivals[i]
        for p in ps:
            one = block(q, e_x, p)
            got(one, xs.at[0], xr.at[at(0, q, p)], to_x)
            if p == 0:
                up_down(1, q, p, 1, t < tp - 1)
                up_down(1, q, p, 0, t > 0)
            n = at(1, q, p)
            send(one, one, cs.at[n], cr.at[n], to_core)

    def take_core(i):
        q = arrivals[i]
        for p in range(pieces):
            got(block(q, e_core, p), cs.at[0], cr.at[at(0, q, p)], to_core)
            got(block(q, e_xc, p), cs.at[0], cr.at[at(1, q, p)], to_core)

    def take_meta():
        got(m.at[e_core], ms.at[1], mr.at[1], to_core)
        got(m.at[e_xc], ms.at[2], mr.at[2], to_core)

    got(m.at[e_x], ms.at[0], mr.at[0], to_x)
    send(m.at[e_x], m.at[e_x], ms.at[2], mr.at[2], to_core)
    take_z(1, [1])
    take_meta()

    slots = pick.shape[0]
    mine = e.astype(f32)
    earlier = (
        lax.broadcasted_iota(jnp.int32, (LANES, LANES), 0)
        < lax.broadcasted_iota(jnp.int32, (LANES, LANES), 1)
    ).astype(b16)
    slot = lax.broadcasted_iota(jnp.int32, (slots, LANES), 0).astype(f32)
    total = jnp.zeros((slots, 1), f32)
    for b in range(ep):
        first, second = m[b, 0:1, :] == mine, m[b, 1:2, :] == mine
        named = jnp.where(first, 1.0, 0.0) + jnp.where(second, 1.0, 0.0)
        weight = jnp.where(first, m[b, 2:3, :], 0.0) + jnp.where(second, m[b, 3:4, :], 0.0)
        spread = jnp.broadcast_to(named, (16, LANES)).astype(b16)
        position = jnp.dot(spread, earlier, preferred_element_type=f32)[0:1, :]
        where_to = jnp.where(named > 0.5, position + float(b * cap), -1.0)
        chosen = jnp.where(slot == where_to, 1.0, 0.0)
        total = total + jnp.sum(chosen * weight, axis=1, keepdims=True)
        pick[:, b * LANES:(b + 1) * LANES] = chosen.astype(b16)
        base = ((b % 2) * half + b // 2) * tok
        place[base:base + tok, :] = chosen.T[0:tok, :].astype(b16)
    scale[...] = jnp.broadcast_to(total, scale.shape)

    step = ff // 2
    acc_g[...] = jnp.zeros(acc_g.shape, f32)
    acc_u[...] = jnp.zeros(acc_u.shape, f32)

    def chosen_at(values, i):
        found = values[0]
        for k in range(1, tp):
            found = jnp.where(i == k, values[k], found)
        return found

    def gather(d):
        q = chosen_at(arrivals, d)
        r = pl.ds(pl.multiple_of(q * feat, feat), feat)
        for k, (src, dst) in enumerate(((gate_hbm, wg), (up_hbm, wu))):
            pltpu.make_async_copy(src.at[0, r, :], dst.at[q], w_sem.at[k * tp + d]).wait()
        everyone = x[q].reshape(ep * x.shape[2], feat)
        packed[...] = jnp.dot(pick[0:rows, :], everyone, preferred_element_type=f32).astype(b16)

    def project(d, cols, last):
        q = chosen_at(arrivals, d)
        g = jnp.dot(packed[...], wg[q, :, cols], preferred_element_type=f32) + acc_g[:, cols]
        u = jnp.dot(packed[...], wu[q, :, cols], preferred_element_type=f32) + acc_u[:, cols]
        if last:
            h = g / (1.0 + jnp.exp(-g)) * u * scale[0:rows, 0:1]
            hidden[:, cols] = h.astype(b16)
        else:
            acc_g[:, cols] = g
            acc_u[:, cols] = u

    take_z(1, bulk[1:])
    take_x(0, bulk)
    take_z(1, [0])
    take_x(0, [0])
    take_core(0)

    def between(n):
        d = (n + 1) // 2
        if n % 2 == 0:
            take_core(d)
            return
        take_z(d + 1, bulk)
        take_x(d, bulk)
        take_z(d + 1, [0])
        take_z(d, [0], 1)

    def half_step(n, carry):
        for k in range(1, 2 * tp - 2):

            @pl.when(n == k)
            def _(k=k):
                between(k)

        @pl.when(n % 2 == 0)
        def _():
            gather(n // 2)

        project(n // 2, pl.ds(pl.multiple_of((n % 2) * step, step), step), False)
        return carry

    lax.fori_loop(0, 2 * tp - 2, half_step, 0)
    take_core(tp - 1)
    gather(tp - 1)
    for j in range(4):
        project(tp - 1, slice(j * ff // 4, (j + 1) * ff // 4), True)

    tail = jnp.zeros((slots - rows, WIDE), b16)
    low, high = slice(0, LANES), slice(LANES, WIDE)

    def to_partner(k):
        away = pl.ds((1 - core) * half, half)
        return rcopy(c.at[k, away], c_in.at[k], rcs.at[k], rcr.at[k], to_core)

    def to_tokens(i, j):
        cols = slice(j * WIDE, (j + 1) * WIDE)
        q = chosen_at(leaving, i)
        part = jnp.dot(hidden[...], wd[q, :, cols], preferred_element_type=f32).astype(b16)
        part = jnp.concatenate([part, tail], axis=0) if slots > rows else part
        back = jnp.dot(place[...], part, preferred_element_type=f32).astype(b16)
        c[i * nt + j] = back.reshape(ep, tok, WIDE)

    def both_cores(k, col, cols=slice(None)):
        return c[k, core * half + col, :, cols].astype(f32) + c_in[k, col, :, cols].astype(f32)

    def in_x(ref, k, first):
        return ref.at[k, :, pl.ds(LANES, LANES)] if first else ref.at[k]

    def to_other_x(k, first):
        return rcopy(in_x(x_out, k, first), in_x(x_in, k, first), rxs.at[k], rxr.at[k], to_x)

    def sum_core(i, j):
        k = i * nt + j
        got(c_in.at[k], rcs.at[0], rcr.at[k], to_core)
        x_out[k] = both_cores(k, 1 - column).astype(b16)

        to_other_x(k, j == 0).start()

    def along(i):
        q = chosen_at(leaving, i)
        right = q > t
        slot_to = jnp.where(~right & (q == t - 1), tp, q)
        return q, slot_to, {"tp": jnp.where(right, lax.rem(t + 1, tp), lax.rem(t + tp - 1, tp))}

    def low_copy(i):
        q, slot_to, peer = along(i)
        return rcopy(y_out.at[i], y_in.at[slot_to], rys.at[i], ryr.at[slot_to], peer)

    def pass_low(i, cond):
        q = chosen_at(leaving, i)

        @pl.when(cond)
        def _():
            @pl.when(~edge)
            def _():
                got(y_in.at[q], rys.at[0], ryr.at[q], above)

            for col in range(half):
                y_out[i, col] = (both_cores(i * nt, col, low) + y_in[q, col].astype(f32)).astype(b16)
            low_copy(i).start()

    def to_own(one):
        @pl.when(t > 0)
        def _():
            one(t)

        @pl.when(t < tp - 1)
        def _():
            one(jnp.int32(tp))

    def to_own_low(at_slot):
        got(y_in.at[at_slot], rys.at[0], ryr.at[at_slot], above)

    def to_own_bulk(j):
        def one(at_slot):
            k = at_slot * nt + j
            got(in_x(z_in, k, j == 0), rzs.at[0], rzr.at[k], above)

        to_own(one)

    def low_sum(col):
        arrived = y_in[t, col].astype(f32) + y_in[tp, col].astype(f32)
        return both_cores((tp - 1) * nt, col, low) + arrived

    def finish_low():
        to_own(to_own_low)
        f_out[...] = low_sum(1 - column).astype(b16)
        send(f_out, f_in, rfs.at[0], rfr.at[0], to_x)

    def sum_x(i, j):
        k, cols = i * nt + j, high if j == 0 else slice(None)
        got(in_x(x_in, k, j == 0), rxs.at[0], rxr.at[k], to_x)
        return both_cores(k, column, cols) + x_in[k, :, cols].astype(f32)

    def bulk_copy(i, j):
        q, slot_to, peer = along(i)
        k, k_to = i * nt + j, slot_to * nt + j
        first = j == 0
        return rcopy(in_x(z_out, k, first), in_x(z_in, k_to, first), rzs.at[k], rzr.at[k_to], peer)

    def pass_on(i, j):
        k, k_in, cols = i * nt + j, chosen_at(leaving, i) * nt + j, high if j == 0 else slice(None)
        value = sum_x(i, j)

        @pl.when(~edge)
        def _():
            got(in_x(z_in, k_in, j == 0), rzs.at[0], rzr.at[k_in], above)

        z_out[k, :, cols] = (value + z_in[k_in, :, cols].astype(f32)).astype(b16)
        bulk_copy(i, j).start()

    def leave(i):
        r = pl.ds(pl.multiple_of(chosen_at(leaving, i) * feat, feat), feat)
        q = chosen_at(leaving, i)
        pltpu.make_async_copy(down_hbm.at[0, :, r], wd.at[q], w_sem.at[2 * tp + i]).wait()

    leave(0)
    for j in range(nt):
        to_tokens(0, j)
    for j in range(nt):
        to_partner(j).start()

    def following(i, carry):
        leave(i)
        for j in range(nt):
            to_tokens(i, j)
        for j in range(nt):
            to_partner(i * nt + j).start()
        for j in range(nt):
            sum_core(i - 1, j)
        pass_low(i - 1, edge)
        return carry

    lax.fori_loop(1, tp, following, 0)

    @pl.when(edge)
    def _():
        for j in range(nt - 1):
            pass_on(0, j)

    for j in range(nt):
        sum_core(tp - 1, j)
    pass_low(0, ~edge)
    for i in range(1, tp - 2):
        pass_low(i, ~edge)

    @pl.when(~edge)
    def _():
        for j in range(nt - 1):
            pass_on(0, j)

    pass_low(tp - 2, ~edge)
    pass_on(0, nt - 1)

    @pl.when(edge)
    def _():
        def by_quarter(i, carry):
            for j in range(nt):
                pass_on(i, j)
            return carry

        lax.fori_loop(1, tp - 1, by_quarter, 0)

    @pl.when(~edge)
    def _():
        for j in range(nt):

            def by_piece(i, carry, j=j):
                pass_on(i, j)
                return carry

            lax.fori_loop(1, tp - 1, by_piece, 0)

    finish_low()
    for j in range(nt):
        cols = high if j == 0 else slice(None)
        start = LANES if j == 0 else j * WIDE
        result = sum_x(tp - 1, j)
        to_own_bulk(j)
        result = result + z_in[t * nt + j, :, cols].astype(f32) + z_in[tp * nt + j, :, cols].astype(f32)
        out[:, start:(j + 1) * WIDE] = result.astype(b16)
    got(f_in, rfs.at[0], rfr.at[0], to_x)
    out[:, low] = (low_sum(column) + f_in[...].astype(f32)).astype(b16)

    def left(src, s):
        rcopy(src, src, s, xr.at[0], to_x).wait_send()

    for n in range(3):
        left(m_own, ms.at[n])
    left(f_out, rfs.at[0])
    left(block(t, e, 0), xs.at[at(0, t, 0)])
    for q in range(tp):
        for p in range(pieces):
            one = block(q, e, p)
            left(one, cs.at[at(0, q, p)])
            left(one, cs.at[at(1, q, p)])
            if p > 0:
                left(one, xs.at[at(0, q, p)])
        for up in (1, 0):

            @pl.when((q <= t) & (t < tp - 1) if up else (q >= t) & (t > 0))
            def _(q=q, up=up):
                for p in range(pieces):
                    left(block(q, e, p), zs.at[at(2 * up, q, p)])
                left(block(q, e_x, 0), zs.at[at(2 * up + 1, q, 0)])

    for i in range(tp):
        for j in range(nt):
            to_partner(i * nt + j).wait_send()
            to_other_x(i * nt + j, j == 0).wait_send()
            if i < tp - 1:
                bulk_copy(i, j).wait_send()
        if i < tp - 1:
            low_copy(i).wait_send()


def kernel_body(tokens, routing, route_gates, expert_gate, expert_up, expert_down):
    ep, tp = lax.axis_size("ep"), lax.axis_size("tp")
    tok, feat = tokens.shape
    ff = expert_gate.shape[2]
    cap = 2 * tok // ep + tok // 16
    rows = up_to(ep * cap, 16)
    slots = up_to(rows, LANES)
    nt, pieces = feat // WIDE, len(row_spans(tok))
    f32, b16 = jnp.float32, jnp.bfloat16
    dma = pltpu.SemaphoreType.DMA
    vmem = pl.BlockSpec(memory_space=pltpu.VMEM)
    hbm = pl.BlockSpec(memory_space=pl.ANY)
    return pl.pallas_call(
        functools.partial(layer_kernel, tp, ep, cap, rows),
        out_shape=pltpu.VMEM((tok, feat), b16),
        in_specs=[hbm, vmem, vmem, hbm, hbm, hbm],
        out_specs=vmem,
        scratch_shapes=[
            pltpu.VMEM((tp, ep, LANES, feat), b16),
            pltpu.VMEM((ep, 8, LANES), f32),
            pltpu.VMEM((8, LANES), f32),
            pltpu.VMEM((slots, ep * LANES), b16),
            pltpu.VMEM((ep * tok, slots), b16),
            pltpu.VMEM((slots, LANES), f32),
            pltpu.VMEM((tp, feat, ff), b16),
            pltpu.VMEM((tp, feat, ff), b16),
            pltpu.VMEM((tp, ff, feat), b16),
            pltpu.VMEM((rows, ff), f32),
            pltpu.VMEM((rows, ff), f32),
            pltpu.VMEM((rows, feat), b16),
            pltpu.VMEM((rows, ff), b16),
            pltpu.VMEM((tp * nt, ep, tok, WIDE), b16),
            pltpu.VMEM((tp * nt, ep // 2, tok, WIDE), b16),
            pltpu.VMEM((tp * nt, tok, WIDE), b16),
            pltpu.VMEM((tp * nt, tok, WIDE), b16),
            pltpu.VMEM((tp, ep // 2, tok, LANES), b16),
            pltpu.VMEM((tp + 1, ep // 2, tok, LANES), b16),
            pltpu.VMEM((tok, LANES), b16),
            pltpu.VMEM((tok, LANES), b16),
            pltpu.VMEM((tp * nt, tok, WIDE), b16),
            pltpu.VMEM(((tp + 1) * nt, tok, WIDE), b16),
            dma((1,)),
            dma((3 * tp,)),
            dma((4 * tp * pieces,)), dma((2 * tp * pieces,)),
            dma((tp * pieces,)), dma((tp * pieces,)),
            dma((2 * tp * pieces,)), dma((2 * tp * pieces,)),
            dma((3,)), dma((3,)),
            dma((tp * nt,)), dma((tp * nt,)),
            dma((tp * nt,)), dma((tp * nt,)),
            dma((tp,)), dma((tp + 1,)),
            dma((1,)), dma((1,)),
            dma((tp * nt,)), dma(((tp + 1) * nt,)),
        ],
        compiler_params=pltpu.CompilerParams(
            collective_id=0, has_side_effects=True, vmem_limit_bytes=60 * 1024 * 1024
        ),
    )(tokens, routing.T, route_gates.T, expert_gate, expert_up, expert_down)


def body(tokens, routing, route_gates, expert_gate, expert_up, expert_down):
    ep, tp = lax.axis_size("ep"), lax.axis_size("tp")
    tok, feat = tokens.shape
    ff = expert_gate.shape[2]
    fits = ep == 4 and 2 < tp < 5 and expert_gate.shape[0] == 1 and 48 <= tok <= LANES and tok % 16 == 0
    fits = fits and feat % WIDE == 0 and ff % 512 == 0 and 3 * tp * feat * ff * 2 <= 40 << 20
    run = kernel_body if fits else plain_body
    return run(tokens, routing, route_gates, expert_gate, expert_up, expert_down)


def solution(mesh):
    return jax.shard_map(
        body,
        mesh=mesh,
        in_specs=(
            P(("rep", "ep"), "tp"),
            P(("rep", "ep"), None),
            P(("rep", "ep"), None),
            P("ep", None, "tp"),
            P("ep", None, "tp"),
            P("ep", "tp", None),
        ),
        out_specs=P(("rep", "ep"), "tp"),
        check_vma=False,
    )
```
